32 devices in a mesh: row: 4 (over z), col: 4 (over x, core), ch: 2 (over y).
Axes of the slice: x: 2, y: 2, z: 4, core: 2. Of those that a mesh axis runs over, the one named last changes fastest.
Arguments:
- image_tokens: bfloat16 [64, 1024, 128], P(('row', 'ch'), 'col'), may hold values from -61 to 61
- labels: int32 [64, 1024], P(('row', 'ch'), 'col'), may hold values from 0 to 2
- rel_index: int32 [64, 64], replicated, may hold values from 0 to 224
- norm_gain: float32 [2, 2, 128], replicated, may hold values from 0.25 to 1.75
- norm_shift: float32 [2, 2, 128], replicated, may hold values from -1.5 to 1.5
- qkv_weight: bfloat16 [2, 3, 128, 128], P(None, None, None, 'ch'), may hold values from -5 to 5
- qkv_bias: float32 [2, 3, 128], P(None, None, 'ch'), may hold values from -1.5 to 1.5
- bias_table: float32 [2, 225, 4], P(None, None, 'ch'), may hold values from -4 to 4
- proj_weight: bfloat16 [2, 128, 128], P(None, 'ch'), may hold values from -0.5 to 0.5
- proj_bias: float32 [2, 128], replicated, may hold values from -1.5 to 1.5
- fc1_weight: bfloat16 [2, 128, 512], P(None, None, 'ch'), may hold values from -0.5 to 0.5
- fc1_bias: float32 [2, 512], P(None, 'ch'), may hold values from -2.5 to 2.5
- fc2_weight: bfloat16 [2, 512, 128], P(None, 'ch'), may hold values from -0.25 to 0.25
- fc2_bias: float32 [2, 128], replicated, may hold values from -1.5 to 1.5
Outputs:
- encoded: bfloat16 [64, 1024, 128], P(('row', 'ch'), 'col')
The draws below stay inside these ranges and needn't reach their ends.
All inputs are finite; a program needn't handle non-finite values.
Results may differ from the reference program's by a relative error of at most 0.014.
Values may be sent and summed in bfloat16 or wider, within the bound.
A program may use at most 128 MiB of HBM per device.

```python
import jax
import jax.numpy as jnp
from jax import lax

C = 128
HEADS = 4
MLP_WIDTH = 512
WIN = 8
SHIFT = 4
TABLE = 225
BLOCKS = 2
KINDS = 3
IMG_ROWS = 64
IMG_COLS = 1024


def draw_image_tokens(key, part):
    base_key = jax.random.fold_in(key, 11)
    values = jnp.clip(jax.random.normal(base_key, (IMG_ROWS, IMG_COLS, C), jnp.float32), -6.0, 6.0)
    return values.astype(jnp.bfloat16)


def draw_qkv_weight(key, part):
    noise_key = jax.random.fold_in(key, 21)
    noise = jnp.clip(jax.random.normal(noise_key, (BLOCKS, 3, C, C), jnp.float32), -4.0, 4.0) * C ** (-0.5)
    return noise.astype(jnp.bfloat16)


def place_ends(values, rng, smallest, high):
    dims = values.shape
    spot = [jax.random.randint(jax.random.fold_in(rng, axis), (), 0, dims[axis]) for axis in range(len(dims))]
    values = values.at[tuple(spot)].set(smallest)
    longest = dims.index(max(dims))
    spot[longest] = (spot[longest] + 1) % dims[longest]
    return values.at[tuple(spot)].set(high)


def steps_of(own_key, extent, shards, low, top_value):
    loudness = 1.0
    for dim, shards_of in shards:
        draws = jax.random.uniform(jax.random.fold_in(jax.random.fold_in(own_key, 6), dim), (shards_of,), jnp.float32, low / len(shards), top_value / len(shards))
        loudness = loudness * jnp.repeat(jnp.exp(draws), extent[dim] // shards_of).reshape((-1,) + (1,) * (len(extent) - 1 - dim))
    return loudness


def scatter_about(rng, extent, scale, bound, shards=(), held_as=jnp.bfloat16):
    drawn = scale * jax.random.normal(rng, extent, jnp.float32)
    if shards:
        drawn = drawn * steps_of(rng, extent, shards, -0.22, 0.18)
    return jnp.clip(drawn, -bound, bound).astype(held_as)


def setup_inputs(seed: int = 0) -> dict:
    arg_keys = jax.random.split(jax.random.key(seed), 15)
    image_tokens = draw_image_tokens(jax.random.fold_in(arg_keys[14], 71), 0)
    labels = place_ends(jax.random.randint(arg_keys[1], (IMG_ROWS, IMG_COLS), 0, KINDS), jax.random.fold_in(arg_keys[1], 1), 0, KINDS - 1).astype(jnp.int32)
    rel_index = place_ends(jax.random.randint(arg_keys[2], (WIN * WIN, WIN * WIN), 0, TABLE), jax.random.fold_in(arg_keys[2], 1), 0, TABLE - 1).astype(jnp.int32)
    norm_gain = jnp.clip(1.0 + 0.15 * jax.random.normal(arg_keys[3], (BLOCKS, 2, C), jnp.float32), 0.25, 1.75)
    norm_shift = scatter_about(arg_keys[4], (BLOCKS, 2, C), 0.3, 1.5, (), jnp.float32)
    qkv_weight = draw_qkv_weight(jax.random.fold_in(arg_keys[14], 71), 0)
    qkv_bias = scatter_about(arg_keys[6], (BLOCKS, 3, C), 0.3, 1.5, ((2, 2),), jnp.float32)
    bias_table = scatter_about(arg_keys[7], (BLOCKS, TABLE, HEADS), 1.0, 4.0, ((2, 2),), jnp.float32)
    proj_weight = scatter_about(arg_keys[8], (BLOCKS, C, C), C ** -0.5, 0.5, ((1, 2),))
    proj_bias = scatter_about(arg_keys[9], (BLOCKS, C), 0.3, 1.5, (), jnp.float32)
    fc1_weight = scatter_about(arg_keys[10], (BLOCKS, C, MLP_WIDTH), C ** -0.5, 0.5, ((2, 2),))
    fc1_bias = scatter_about(arg_keys[11], (BLOCKS, MLP_WIDTH), 0.5, 2.5, ((1, 2),), jnp.float32)
    fc2_weight = scatter_about(arg_keys[12], (BLOCKS, MLP_WIDTH, C), MLP_WIDTH ** -0.5, 0.25, ((1, 2),))
    fc2_bias = scatter_about(arg_keys[13], (BLOCKS, C), 0.3, 1.5, (), jnp.float32)
    return {"image_tokens": image_tokens, "labels": labels, "rel_index": rel_index, "norm_gain": norm_gain, "norm_shift": norm_shift, "qkv_weight": qkv_weight, "qkv_bias": qkv_bias, "bias_table": bias_table, "proj_weight": proj_weight, "proj_bias": proj_bias, "fc1_weight": fc1_weight, "fc1_bias": fc1_bias, "fc2_weight": fc2_weight, "fc2_bias": fc2_bias}


EPS = 1e-05

def layer_norm(values, gain, offset):
    widened = values.astype(jnp.float32)
    center = widened - lax.optimization_barrier(jnp.mean(widened, axis=-1, keepdims=True))
    spread = lax.optimization_barrier(jnp.mean(center * center, axis=-1, keepdims=True))
    return (center * lax.rsqrt(spread + EPS) * gain + offset).astype(jnp.bfloat16)

def position_bias(rel_index, table):
    entries = table.shape[0]
    onehot = (rel_index.reshape(-1, 1) == jnp.arange(entries, dtype=jnp.int32)[None, :]).astype(jnp.float32)
    picked = jnp.dot(onehot, table, precision=lax.Precision.HIGHEST, preferred_element_type=jnp.float32)
    length = rel_index.shape[0]
    return picked.T.reshape(table.shape[1], length, length)

def window_attention(triple, region, bias):
    rows, cols = (triple.shape[0], triple.shape[1])
    width = triple.shape[3]
    heads = bias.shape[0]
    depth = width // heads
    across = rows // WIN
    along = cols // WIN
    grid = triple.reshape(across, WIN, along, WIN, 3, heads, depth)
    grid = grid.transpose(0, 2, 4, 5, 1, 3, 6).reshape(across, along, 3, heads, WIN * WIN, depth)
    grid = grid.astype(jnp.float32)
    scores = jnp.einsum('abhpd,abhqd->abhpq', grid[:, :, 0], grid[:, :, 1])
    scores = scores * depth ** (-0.5) + bias
    if region is not None:
        window_ids = region.reshape(across, WIN, along, WIN).transpose(0, 2, 1, 3).reshape(across, along, WIN * WIN)
        allowed = window_ids[:, :, :, None] == window_ids[:, :, None, :]
        scores = jnp.where(allowed[:, :, None], scores, -jnp.inf)
    highest = lax.optimization_barrier(jnp.max(scores, axis=-1, keepdims=True))
    raised = jnp.exp(scores - highest)
    weights = (raised / lax.optimization_barrier(jnp.sum(raised, axis=-1, keepdims=True))).astype(jnp.bfloat16)
    mixed = jnp.einsum('abhpq,abhqd->abhpd', weights.astype(jnp.float32), grid[:, :, 2])
    mixed = mixed.astype(jnp.bfloat16).reshape(across, along, heads, WIN, WIN, depth)
    return mixed.transpose(0, 3, 1, 4, 2, 5).reshape(rows, cols, width)

def attend_image(triple, region, bias, offset):
    rolled = jnp.roll(triple, (-offset, -offset), axis=(0, 1))
    bands = rolled.reshape(IMG_ROWS // WIN, WIN, IMG_COLS, 3, C)
    if region is None:
        result = lax.map(lambda band: window_attention(band, None, bias), bands)
    else:
        region_bands = jnp.roll(region, (-offset, -offset), axis=(0, 1)).reshape(IMG_ROWS // WIN, WIN, IMG_COLS)
        result = lax.map(lambda pair: window_attention(pair[0], pair[1], bias), (bands, region_bands))
    result = result.reshape(IMG_ROWS, IMG_COLS, C)
    return jnp.roll(result, (offset, offset), axis=(0, 1))

def swin_block(tokens, block, region, offset, norm_gain, norm_shift, qkv_weight, qkv_bias, bias_table, proj_weight, proj_bias, fc1_weight, fc1_bias, fc2_weight, fc2_bias, rel_index):
    normed = layer_norm(tokens, norm_gain[block, 0], norm_shift[block, 0])
    stacked = qkv_weight[block].transpose(1, 0, 2).reshape(C, 3 * C)
    triple = jnp.dot(normed.reshape(-1, C), stacked, preferred_element_type=jnp.float32)
    triple = (triple.reshape(IMG_ROWS, IMG_COLS, 3, C) + qkv_bias[block]).astype(jnp.bfloat16)
    bias = position_bias(rel_index, bias_table[block])
    attended = attend_image(triple, region, bias, offset)
    mixed = jnp.dot(attended.reshape(-1, C), proj_weight[block], preferred_element_type=jnp.float32)
    middle = (tokens.astype(jnp.float32) + mixed.reshape(IMG_ROWS, IMG_COLS, C) + proj_bias[block]).astype(jnp.bfloat16)

    def feed(band):
        normed_two = layer_norm(band, norm_gain[block, 1], norm_shift[block, 1])
        inner = jnp.dot(normed_two.reshape(-1, C), fc1_weight[block], preferred_element_type=jnp.float32)
        hidden = jax.nn.gelu(inner + fc1_bias[block], approximate=False).astype(jnp.bfloat16)
        outer = jnp.dot(hidden, fc2_weight[block], preferred_element_type=jnp.float32).reshape(band.shape)
        return (band.astype(jnp.float32) + outer + fc2_bias[block]).astype(jnp.bfloat16)
    result = lax.map(feed, middle.reshape(IMG_ROWS // WIN, WIN, IMG_COLS, C))
    return result.reshape(IMG_ROWS, IMG_COLS, C)

def reference(image_tokens, labels, rel_index, norm_gain, norm_shift, qkv_weight, qkv_bias, bias_table, proj_weight, proj_bias, fc1_weight, fc1_bias, fc2_weight, fc2_bias):
    grid_rows = jnp.arange(IMG_ROWS, dtype=jnp.int32)
    grid_cols = jnp.arange(IMG_COLS, dtype=jnp.int32)
    region = labels * 4 + (grid_rows < SHIFT).astype(jnp.int32)[:, None] * 2 + (grid_cols < SHIFT).astype(jnp.int32)[None, :]
    current = image_tokens
    for block in range(BLOCKS):
        if block % 2 == 1:
            current = swin_block(current, block, region, SHIFT, norm_gain, norm_shift, qkv_weight, qkv_bias, bias_table, proj_weight, proj_bias, fc1_weight, fc1_bias, fc2_weight, fc2_bias, rel_index)
        else:
            current = swin_block(current, block, None, 0, norm_gain, norm_shift, qkv_weight, qkv_bias, bias_table, proj_weight, proj_bias, fc1_weight, fc1_bias, fc2_weight, fc2_bias, rel_index)
    return current
```

```python
import functools
import math

import jax
import jax.numpy as jnp
from jax import lax
from jax.experimental import pallas as pl
from jax.experimental.pallas import tpu as pltpu
from jax.sharding import PartitionSpec as P

WIN = 8
SHIFT = 4
BLOCKS = 2
EPS = 1e-05
FAR = -1e30
CLASSES = 16
bf16 = jnp.bfloat16
f32 = jnp.float32


def padded(shard, sides, width):
    for axis, dim in sides:
        size, length = (lax.axis_size(axis), shard.shape[dim])
        up = [(i, (i + 1) % size) for i in range(size)]
        down = [(j, i) for i, j in up]
        last = lax.slice_in_dim(shard, length - width, length, axis=dim)
        leading = lax.slice_in_dim(shard, 0, width, axis=dim)
        before = lax.ppermute(last, axis, up)
        after = lax.ppermute(leading, axis, down)
        shard = jnp.concatenate([before, shard, after], axis=dim)
    return shard


def position_bias(rel_index, table):
    entries = table.shape[0]
    onehot = (rel_index.reshape(-1, 1) == jnp.arange(entries, dtype=jnp.int32)[None, :]).astype(f32)
    picked = jnp.dot(onehot, table, precision=lax.Precision.HIGHEST, preferred_element_type=f32)
    length = rel_index.shape[0]
    return picked.T.reshape(table.shape[1], length, length)


def dot(a, b):
    return jnp.dot(a, b, preferred_element_type=f32)


def dot_t(a, b):
    return lax.dot_general(a, b, (((1,), (1,)), ((), ())), preferred_element_type=f32)


def layer_norm(x, gain, offset):
    center = x - jnp.mean(x, axis=-1, keepdims=True)
    spread = jnp.mean(center * center, axis=-1, keepdims=True)
    return (center * lax.rsqrt(spread + EPS) * gain + offset).astype(bf16)


def rows_of(x):
    return x.reshape(x.shape[0] * x.shape[1], x.shape[2])


def attend(q, k, v, hmask, bias, heads, depth, far=None):
    keys = k.shape[0]
    kb = jnp.concatenate([k] * heads, axis=0) * hmask
    vb = jnp.concatenate([v] * heads, axis=0) * hmask
    if far is not None:
        fq, fk = far
        q = jnp.concatenate([q, fq], axis=1)
        kb = jnp.concatenate([kb, jnp.concatenate([fk] * heads, axis=0)], axis=1)
    s = dot_t(q, kb) * (depth ** (-0.5)) + bias
    per = 128 // keys
    parts = []
    lane = lax.broadcasted_iota(jnp.int32, (s.shape[0], 128), 1)
    for c in range(0, s.shape[1], 128):
        t = s[:, c : c + 128]
        top = None
        for j in range(per):
            inside = (lane >= j * keys) & (lane < (j + 1) * keys)
            peak = jnp.max(jnp.where(inside, t, -jnp.inf), axis=-1, keepdims=True)
            top = peak if top is None else jnp.where(lane >= j * keys, peak, top)
        parts.append(jnp.exp(t - top))
    p = jnp.concatenate(parts, axis=1).astype(bf16)
    o = dot(p, jnp.concatenate([vb, hmask], axis=1))
    width = q.shape[1] if far is None else k.shape[1]
    return (o[:, :width] / o[:, width:]).astype(bf16)


def finish(x, attended, w, b):
    mixed = dot(attended, w["proj"][b])
    middle = (x + mixed + w["proj_b"][b]).astype(bf16).astype(f32)
    normed = layer_norm(middle, w["gain"][b][1:2], w["shift"][b][1:2])
    inner = dot(normed, w["fc1"][b]) + w["fc1_b"][b]
    hidden = (0.5 * inner * (1.0 + lax.erf(inner * (0.5 ** 0.5)))).astype(bf16)
    outer = dot(hidden, w["fc2"][b])
    return (middle + outer + w["fc2_b"][b]).astype(bf16)


NAMES = ("gain", "shift", "qkv", "qkv_b", "bias", "proj", "proj_b", "fc1", "fc1_b", "fc2", "fc2_b")


def head_mask(heads, keys, width):
    depth = width // heads
    row = lax.broadcasted_iota(jnp.int32, (heads * keys, width), 0) // keys
    col = lax.broadcasted_iota(jnp.int32, (heads * keys, width), 1) // depth
    return (row == col).astype(f32).astype(bf16)


def qkv_of(x, w, b):
    normed = layer_norm(x, w["gain"][b][0:1], w["shift"][b][0:1])
    return dot(normed, w["qkv"][b]) + w["qkv_b"][b]


def first_chunk(x, w, heads, hmask):
    rows, wide, width = x.shape
    depth = width // heads
    toks = jnp.concatenate(
        [rows_of(x[:, c : c + WIN]) for c in range(0, wide, WIN)], axis=0
    )
    triple = qkv_of(toks, w, 0)
    outs = []
    n = WIN * WIN
    for g in range(wide // WIN):
        t = triple[g * n : (g + 1) * n].astype(bf16)
        outs.append(
            attend(t[:, :width], t[:, width : 2 * width], t[:, 2 * width :], hmask, w["bias"][0], heads, depth)
        )
    return finish(toks, jnp.concatenate(outs, axis=0), w, 0)


def kernel0(heads, chunk, x_ref, *refs):
    w = dict(zip(NAMES, refs[: len(NAMES)]))
    o_ref = refs[len(NAMES)]
    rows, cols, width = x_ref.shape
    hmask = head_mask(heads, WIN * WIN, width)

    def body(i, _):
        at = pl.ds(pl.multiple_of(i * chunk, chunk), chunk)
        y = first_chunk(x_ref[:, at, :].astype(f32), w, heads, hmask).astype(f32)
        n = WIN * WIN
        y = jnp.concatenate(
            [y[g * n : (g + 1) * n].reshape(WIN, WIN, width) for g in range(chunk // WIN)], axis=1
        )
        o_ref[:, at, :] = y.astype(bf16)
        return 0

    lax.fori_loop(0, cols // chunk, body, 0)


def second_chunk(x, fq, fk, w, heads, hmask):
    rows, wide, width = x.shape
    depth = width // heads
    half = WIN // 2
    outs, toks = [], []
    n = WIN * WIN
    for r in range(0, rows, WIN):
        xs = [rows_of(x[r : r + WIN, c : c + WIN]) for c in range(0, wide, WIN)]
        fqs = [rows_of(fq[r : r + WIN, c : c + WIN]) for c in range(0, wide, WIN)]
        fks = [rows_of(fk[r : r + WIN, c : c + WIN]) for c in range(0, wide, WIN)]
        triple = qkv_of(jnp.concatenate(xs, axis=0), w, 1)
        own = slice(half * WIN, n) if r == 0 else slice(0, half * WIN)
        bias = w["bias"][1][own, :]
        for g in range(wide // WIN):
            t = triple[g * n : (g + 1) * n].astype(bf16)
            outs.append(
                attend(
                    t[own, :width], t[:, width : 2 * width], t[:, 2 * width :], hmask, bias, heads, depth,
                    (fqs[g][own].astype(bf16), fks[g].astype(bf16)),
                )
            )
            toks.append(xs[g][own])
    return finish(jnp.concatenate(toks, axis=0), jnp.concatenate(outs, axis=0), w, 1)


def kernel1(heads, chunk, x_ref, reg_ref, *refs):
    w = dict(zip(NAMES, refs[: len(NAMES)]))
    o_ref, ext, fqr, fkr, res = refs[len(NAMES) :]
    rows, wide, width = x_ref.shape
    hmask = head_mask(heads, WIN * WIN, width)
    ext[...] = x_ref[...].astype(f32)
    lanes = reg_ref.shape[1]
    kinds = lax.broadcasted_iota(jnp.int32, (128, lanes), 0)
    for r in range(rows):
        same = (reg_ref[r : r + 1, :] == kinds).astype(f32).T[:wide]
        fqr[r] = same * FAR
        fkr[r] = 1.0 - same
    half = WIN // 2

    def body(i, _):
        at = pl.ds(pl.multiple_of(i * chunk, WIN), chunk)
        y = second_chunk(ext[:, at, :], fqr[:, at, :], fkr[:, at, :], w, heads, hmask).astype(f32)
        n = half * WIN
        g = chunk // WIN
        for r in range(2):
            for j in range(g):
                k = (r * g + j) * n
                col = pl.ds(pl.multiple_of(i * chunk + j * WIN, WIN), WIN)
                res[r * half : (r + 1) * half, col, :] = y[k : k + n].reshape(half, WIN, width)
        return 0

    lax.fori_loop(0, wide // chunk, body, 0)
    o_ref[...] = res[:, SHIFT : SHIFT + o_ref.shape[1], :].astype(bf16)


def chunk_of(windows, most):
    return max(d for d in range(1, most + 1) if windows % d == 0) * WIN


def on_device(
    image_tokens, labels, rel_index, norm_gain, norm_shift, qkv_weight, qkv_bias, bias_table,
    proj_weight, proj_bias, fc1_weight, fc1_bias, fc2_weight, fc2_bias,
):
    own_rows, tile_cols, width = image_tokens.shape
    groups = lax.axis_size("ch")
    first_row = (lax.axis_index("row") * groups + lax.axis_index("ch")) * own_rows
    image_rows = own_rows * groups * lax.axis_size("row")
    image_cols = tile_cols * lax.axis_size("col")
    margin = padded(labels, ((("row", "ch"), 0), ("col", 1)), SHIFT)
    grid_rows = jnp.mod(first_row - SHIFT + jnp.arange(own_rows + 2 * SHIFT, dtype=jnp.int32), image_rows)
    grid_cols = jnp.mod(
        lax.axis_index("col") * tile_cols - SHIFT + jnp.arange(tile_cols + 2 * SHIFT, dtype=jnp.int32), image_cols
    )
    region = (
        margin * 4
        + (grid_rows < SHIFT).astype(jnp.int32)[:, None] * 2
        + (grid_cols < SHIFT).astype(jnp.int32)[None, :]
    )
    region = jnp.pad(region, ((0, 0), (0, -region.shape[1] % 128)))
    qkv = lax.all_gather(qkv_weight, "ch", axis=3, tiled=True)
    proj = lax.all_gather(proj_weight, "ch", axis=1, tiled=True)
    fc1 = lax.all_gather(fc1_weight, "ch", axis=2, tiled=True)
    fc2 = lax.all_gather(fc2_weight, "ch", axis=1, tiled=True)
    qkv_b = lax.all_gather(qkv_bias, "ch", axis=2, tiled=True)
    table = lax.all_gather(bias_table, "ch", axis=2, tiled=True)
    fc1_b = lax.all_gather(fc1_bias, "ch", axis=1, tiled=True)
    heads = table.shape[2]
    n = WIN * WIN
    bias = jnp.stack([
        position_bias(rel_index, table[b]).transpose(1, 0, 2).reshape(n, heads * n) for b in range(BLOCKS)
    ])
    weights = (
        norm_gain, norm_shift,
        qkv.transpose(0, 2, 1, 3).reshape(BLOCKS, width, 3 * width), qkv_b.reshape(BLOCKS, 1, 3 * width),
        bias, proj, proj_bias[:, None], fc1, fc1_b[:, None], fc2, fc2_bias[:, None],
    )
    vmem = pl.BlockSpec(memory_space=pltpu.VMEM)
    params = pltpu.CompilerParams(vmem_limit_bytes=60 * 1024 * 1024)
    x1 = pl.pallas_call(
        functools.partial(kernel0, heads, chunk_of(tile_cols // WIN, 8)),
        out_shape=jax.ShapeDtypeStruct(image_tokens.shape, bf16),
        in_specs=[vmem] * (1 + len(weights)),
        out_specs=vmem,
        compiler_params=params,
        name="regular",
    )(image_tokens, *weights)
    ext = padded(x1, ((("row", "ch"), 0), ("col", 1)), SHIFT)
    return pl.pallas_call(
        functools.partial(kernel1, heads, chunk_of(tile_cols // WIN + 1, 11)),
        out_shape=jax.ShapeDtypeStruct(image_tokens.shape, bf16),
        in_specs=[vmem] * (2 + len(weights)),
        out_specs=vmem,
        scratch_shapes=[
            pltpu.VMEM(ext.shape, f32),
            pltpu.VMEM(ext.shape[:2] + (128,), f32),
            pltpu.VMEM(ext.shape[:2] + (128,), f32),
            pltpu.VMEM((own_rows,) + ext.shape[1:], f32),
        ],
        compiler_params=params,
        name="shifted",
    )(ext, region, *weights)


def solution(mesh):
    in_specs = (
        P(("row", "ch"), "col", None), P(("row", "ch"), "col"), P(), P(), P(),
        P(None, None, None, "ch"), P(None, None, "ch"), P(None, None, "ch"), P(None, "ch", None), P(),
        P(None, None, "ch"), P(None, "ch"), P(None, "ch", None), P(),
    )
    out_specs = P(("row", "ch"), "col", None)
    return jax.shard_map(on_device, mesh=mesh, in_specs=in_specs, out_specs=out_specs, check_vma=False)
```

```python
import functools

import jax
import jax.numpy as jnp
from jax import lax
from jax.experimental import pallas as pl
from jax.experimental.pallas import tpu as pltpu
from jax.sharding import PartitionSpec as P

WIN = 8
SHIFT = 4
BLOCKS = 2
EPS = 1e-05
FAR = -1e30
bf16 = jnp.bfloat16
f32 = jnp.float32


def dot(a, b):
    return jnp.dot(a, b, preferred_element_type=f32)


def dot_t(a, b):
    return lax.dot_general(a, b, (((1,), (1,)), ((), ())), preferred_element_type=f32)


def layer_norm(x, gain, offset):
    center = x - jnp.mean(x, axis=-1, keepdims=True)
    spread = jnp.mean(center * center, axis=-1, keepdims=True)
    return (center * lax.rsqrt(spread + EPS) * gain + offset).astype(bf16)


def rows_of(x):
    return x.reshape(x.shape[0] * x.shape[1], x.shape[2])


def attend(q, k, v, hmask, bias, heads, depth, far=None):
    keys = k.shape[0]
    kb = jnp.concatenate([k] * heads, axis=0) * hmask
    vb = jnp.concatenate([v] * heads, axis=0) * hmask
    if far is not None:
        fq, fk = far
        q = jnp.concatenate([q, fq], axis=1)
        kb = jnp.concatenate([kb, jnp.concatenate([fk] * heads, axis=0)], axis=1)
    s = dot_t(q, kb) * (depth ** (-0.5)) + bias
    per = 128 // keys
    parts = []
    lane = lax.broadcasted_iota(jnp.int32, (s.shape[0], 128), 1)
    for c in range(0, s.shape[1], 128):
        t = s[:, c : c + 128]
        top = None
        for j in range(per):
            inside = (lane >= j * keys) & (lane < (j + 1) * keys)
            peak = jnp.max(jnp.where(inside, t, -jnp.inf), axis=-1, keepdims=True)
            top = peak if top is None else jnp.where(lane >= j * keys, peak, top)
        parts.append(jnp.exp(t - top))
    p = jnp.concatenate(parts, axis=1).astype(bf16)
    o = dot(p, jnp.concatenate([vb, hmask], axis=1))
    width = q.shape[1] if far is None else k.shape[1]
    return (o[:, :width] / o[:, width:]).astype(bf16)


def finish(x, attended, w, b):
    mixed = dot(attended, w["proj"][b])
    middle = (x + mixed + w["proj_b"][b]).astype(bf16).astype(f32)
    normed = layer_norm(middle, w["gain"][b][1:2], w["shift"][b][1:2])
    inner = dot(normed, w["fc1"][b]) + w["fc1_b"][b]
    hidden = (0.5 * inner * (1.0 + lax.erf(inner * (0.5 ** 0.5)))).astype(bf16)
    outer = dot(hidden, w["fc2"][b])
    return (middle + outer + w["fc2_b"][b]).astype(bf16)


def head_mask(heads, keys, width):
    depth = width // heads
    row = lax.broadcasted_iota(jnp.int32, (heads * keys, width), 0) // keys
    col = lax.broadcasted_iota(jnp.int32, (heads * keys, width), 1) // depth
    return (row == col).astype(f32).astype(bf16)


def qkv_of(x, w, b):
    normed = layer_norm(x, w["gain"][b][0:1], w["shift"][b][0:1])
    return dot(normed, w["qkv"][b]) + w["qkv_b"][b]


def first_chunk(x, w, heads, hmask):
    rows, wide, width = x.shape
    depth = width // heads
    toks = jnp.concatenate(
        [rows_of(x[:, c : c + WIN]) for c in range(0, wide, WIN)], axis=0
    )
    triple = qkv_of(toks, w, 0)
    outs = []
    n = WIN * WIN
    for g in range(wide // WIN):
        t = triple[g * n : (g + 1) * n].astype(bf16)
        outs.append(
            attend(t[:, :width], t[:, width : 2 * width], t[:, 2 * width :], hmask, w["bias"][0], heads, depth)
        )
    return finish(toks, jnp.concatenate(outs, axis=0), w, 0)


def second_chunk(x, reg, w, heads, hmask):
    kinds = lax.broadcasted_iota(jnp.int32, (WIN * WIN, 128), 1).astype(f32)
    rows, wide, width = x.shape
    depth = width // heads
    half = WIN // 2
    outs, toks = [], []
    n = WIN * WIN
    for r in range(0, rows, WIN):
        xs = [rows_of(x[r : r + WIN, c : c + WIN]) for c in range(0, wide, WIN)]
        same = [(rows_of(reg[r : r + WIN, c : c + WIN]) == kinds).astype(f32) for c in range(0, wide, WIN)]
        triple = qkv_of(jnp.concatenate(xs, axis=0), w, 1)
        own = slice(half * WIN, n) if r == 0 else slice(0, half * WIN)
        bias = w["bias"][1][own, :]
        for g in range(wide // WIN):
            t = triple[g * n : (g + 1) * n].astype(bf16)
            outs.append(
                attend(
                    t[own, :width], t[:, width : 2 * width], t[:, 2 * width :], hmask, bias, heads, depth,
                    ((same[g][own] * FAR).astype(bf16), (1.0 - same[g]).astype(bf16)),
                )
            )
            toks.append(xs[g][own])
    return finish(jnp.concatenate(toks, axis=0), jnp.concatenate(outs, axis=0), w, 1)


def fused(
    heads, chunk0, chunk1,
    x_ref, lab_ref, rel_ref, gain, shift, qkv_w, qkv_b, table, proj_w, proj_b, fc1_w, fc1_b, fc2_w, fc2_b,
    o_ref,
    ext, regb, res, x1, top, bot, side, corner, lab, tsc, tab_own, tab_all,
    qkv_all, qb_all, f1b_all, qkv, qb, bias, proj, fc1, f1b, fc2,
    wsend, wrecv, rsend, rrecv, lsend, lrecv, hsend, hrecv, esend, erecv, own_sem,
):
    rows, cols, width = x_ref.shape
    n = lax.axis_size("ch")
    nrow, ncol = lax.axis_size("row"), lax.axis_size("col")
    row, col, ch = lax.axis_index("row"), lax.axis_index("col"), lax.axis_index("ch")
    ring = row * n + ch
    total = nrow * n

    def at(dr, dc):
        p = lax.rem(ring + dr + total, total)
        return (p // n, lax.rem(col + dc + ncol, ncol), lax.rem(p, n))

    around = [(-1, -1), (-1, 0), (-1, 1), (0, -1), (0, 1), (1, -1), (1, 0), (1, 1)]
    peers = [(row, col, lax.rem(ch + d, n)) for d in range(1, n)]
    mate = (row, col + 1 - 2 * lax.rem(col, 2), ch)
    core = lax.rem(col, 2)
    mesh_id = pl.DeviceIdType.MESH

    barrier = pltpu.get_barrier_semaphore()
    targets = [at(*d) for d in around] + peers + [mate]
    for t in targets:
        pl.semaphore_signal(barrier, inc=1, device_id=t, device_id_type=mesh_id)

    def remote(src, dst, ssem, rsem, to):
        return pltpu.make_async_remote_copy(
            src_ref=src, dst_ref=dst, send_sem=ssem, recv_sem=rsem, device_id=to, device_id_type=mesh_id
        )

    for b in range(BLOCKS):
        tsc[...] = jnp.zeros_like(tsc)
        tsc[: table.shape[1], : table.shape[2]] = table[b]
        tab_own[b] = tsc[...].T[:8]
    pl.semaphore_wait(barrier, len(targets))

    kh, ph, fh, gh = width // 2, proj_w.shape[1] // 2, width // 2, fc2_w.shape[1] // 2
    pw, fw, gw = proj_w.shape[1], fc1_w.shape[2], fc2_w.shape[1]

    def pieces(b, owner):
        k0, p0, f0, g0 = (pl.multiple_of(core * v, 16) for v in (kh, ph, fh, gh))
        return [
            (qkv_w.at[b, :, pl.ds(k0, kh), :], qkv_all.at[owner, b, :, pl.ds(k0, kh), :]),
            (proj_w.at[b, pl.ds(p0, ph), :], proj.at[b, pl.ds(pl.multiple_of(owner * pw + p0, 16), ph), :]),
            (
                fc1_w.at[b, pl.ds(f0, fh), :],
                fc1.at[b, pl.ds(f0, fh), pl.ds(pl.multiple_of(owner * fw, 128), fw)],
            ),
            (fc2_w.at[b, pl.ds(g0, gh), :], fc2.at[b, pl.ds(pl.multiple_of(owner * gw + g0, 16), gh), :]),
        ]

    direct, relays, smalls = {}, {}, []
    for d in range(1, n):
        to, owner = peers[d - 1], lax.rem(ch - d + n, n)
        for b in range(BLOCKS):
            for i, (src, dst) in enumerate(pieces(b, ch)):
                direct[d, b, i] = remote(src, dst, wsend.at[d - 1, b, i], wrecv.at[d - 1, b, i], to)
            for i, (_, dst) in enumerate(pieces(b, owner)):
                relays[d, b, i] = remote(dst, dst, rsend.at[d - 1, b, i], rrecv.at[d - 1, b, i], mate)
        for i, (src, dst) in enumerate(
            [(tab_own, tab_all.at[ch]), (qkv_b, qb_all.at[ch]), (fc1_b, f1b_all.at[ch])]
        ):
            smalls.append(remote(src, dst, wsend.at[d - 1, BLOCKS, i], wrecv.at[d - 1, BLOCKS, i], to))
    for c in smalls:
        c.start()
    for b in range(BLOCKS):
        for d in range(1, n):
            for i in range(4):
                direct[d, b, i].start()
    labels = []
    for i, d in enumerate(around):
        labels.append(remote(lab_ref, lab.at[i], lsend.at[i], lrecv.at[i], at(-d[0], -d[1])))
        labels[-1].start()
    locals_ = [
        (qkv_w, qkv_all.at[ch]),
        (proj_w, proj.at[:, pl.ds(pl.multiple_of(ch * pw, 16), pw), :]),
        (fc1_w, fc1.at[:, :, pl.ds(pl.multiple_of(ch * fw, 128), fw)]),
        (fc2_w, fc2.at[:, pl.ds(pl.multiple_of(ch * gw, 16), gw), :]),
        (tab_own, tab_all.at[ch]), (qkv_b, qb_all.at[ch]), (fc1_b, f1b_all.at[ch]),
    ]
    locals_ = [pltpu.make_async_copy(s, d, own_sem.at[i]) for i, (s, d) in enumerate(locals_)]
    for c in locals_:
        c.start()
    for c in locals_:
        c.wait()
    for c in smalls:
        c.wait()

    part = width // n
    keys = WIN * WIN
    for j in range(n):
        for b in range(BLOCKS):
            for m in range(3):
                qb[b, :, m * width + j * part : m * width + (j + 1) * part] = qb_all[j, b, m : m + 1, :]
            f1b[b, :, j * fw : (j + 1) * fw] = f1b_all[j, b : b + 1, :]
    local_heads = table.shape[2]
    per = 128 // keys
    idx = jnp.concatenate([rel_ref[...]] * per, axis=1)
    lane = lax.broadcasted_iota(jnp.int32, idx.shape, 1)
    for b in range(BLOCKS):
        for t in range(heads // per):
            out = None
            for j in range(per):
                h = t * per + j
                entry = tab_all[h // local_heads, b, h % local_heads : h % local_heads + 1, :]
                got = None
                for c in range(0, entry.shape[1], 128):
                    piece = jnp.broadcast_to(entry[:, c : c + 128], idx.shape)
                    here = jnp.take_along_axis(piece, idx & 127, axis=1, mode="promise_in_bounds")
                    got = here if got is None else jnp.where(idx >= c, here, got)
                out = got if out is None else jnp.where(lane >= j * keys, got, out)
            bias[b, :, t * 128 : (t + 1) * 128] = out

    def bring(b):
        for d in range(1, n):
            for i in range(4):
                direct[d, b, i].wait_recv()
                relays[d, b, i].start()

    def settle(b):
        for d in range(1, n):
            for i in range(4):
                relays[d, b, i].wait_recv()
        for j in range(n):
            for m in range(3):
                qkv[b, :, m * width + j * part : m * width + (j + 1) * part] = qkv_all[j, b, m]

    for c in labels:
        c.wait()
    def column(up, mid, down):
        return jnp.concatenate([up[rows - SHIFT :], mid, down[:SHIFT]], axis=0)
    west = column(lab[0], lab[3], lab[5]).astype(f32)
    mid = column(lab[1], lab_ref[...], lab[6]).astype(f32)
    east = column(lab[2], lab[4], lab[7]).astype(f32)
    tall = rows + 2 * SHIFT
    moved = pltpu.roll(jnp.concatenate([mid, jnp.zeros((tall, 128), f32)], axis=1), SHIFT, 1)
    span = cols + 128
    j = lax.broadcasted_iota(jnp.int32, (tall, span), 1)
    i = lax.broadcasted_iota(jnp.int32, (tall, span), 0)
    blank = jnp.zeros((tall, span - 128), f32)
    left = jnp.concatenate([pltpu.roll(west[:, cols - 128 :], SHIFT, 1), blank], axis=1)
    right = jnp.concatenate([blank, pltpu.roll(east[:, :128], SHIFT, 1)], axis=1)
    kind = jnp.where(j < SHIFT, left, jnp.where(j < cols + SHIFT, moved, right))
    def flag(here, when):
        return jnp.where(here, when.astype(f32), 0.0)
    low = flag((i >= SHIFT) & (i < 2 * SHIFT), ring == 0) + flag(i >= rows + SHIFT, ring == total - 1)
    front = flag((j >= SHIFT) & (j < 2 * SHIFT), col == 0) + flag(j >= cols + SHIFT, col == ncol - 1)
    kind = kind * 4.0 + low * 2.0 + front
    turned = kind.T[: cols + 2 * SHIFT].astype(bf16)
    pick = lax.broadcasted_iota(jnp.int32, (tall, 128), 0)
    for r in range(tall):
        regb[r] = dot(turned, (pick == r).astype(f32).astype(bf16))

    bring(0)
    bring(1)
    settle(0)

    w = {
        "gain": gain, "shift": shift, "qkv": qkv, "qkv_b": qb, "bias": bias, "proj": proj,
        "proj_b": [proj_b[b : b + 1] for b in range(BLOCKS)], "fc1": fc1, "fc1_b": f1b, "fc2": fc2,
        "fc2_b": [fc2_b[b : b + 1] for b in range(BLOCKS)],
    }
    hmask = head_mask(heads, keys, width)

    def halo(k):
        span = pl.ds(pl.multiple_of(k * chunk0, chunk0), chunk0)
        return [
            remote(x1.at[rows - SHIFT :, span, :], top.at[:, span, :], hsend.at[0, k], hrecv.at[0, k], at(1, 0)),
            remote(x1.at[:SHIFT, span, :], bot.at[:, span, :], hsend.at[1, k], hrecv.at[1, k], at(-1, 0)),
        ]

    def regular(k, _):
        span = pl.ds(pl.multiple_of(k * chunk0, chunk0), chunk0)
        y = first_chunk(x_ref[:, span, :].astype(f32), w, heads, hmask).astype(f32)
        m = WIN * WIN
        y = jnp.concatenate(
            [y[g * m : (g + 1) * m].reshape(WIN, WIN, width) for g in range(chunk0 // WIN)], axis=1
        )
        x1[:, span, :] = y.astype(bf16)
        for c in halo(k):
            c.start()
        return 0

    lax.fori_loop(0, cols // chunk0, regular, 0)
    edge = side.shape[2]
    edges = []
    for s, dc in ((0, 1), (1, -1)):
        span = slice(cols - edge, cols) if dc == 1 else slice(0, edge)
        edges.append(remote(x1.at[:, span, :], side.at[s], esend.at[s, 0], erecv.at[s, 0], at(0, dc)))
        edges.append(
            remote(x1.at[rows - SHIFT :, span, :], corner.at[s, 0], esend.at[s, 1], erecv.at[s, 1], at(1, dc))
        )
        edges.append(remote(x1.at[:SHIFT, span, :], corner.at[s, 1], esend.at[s, 2], erecv.at[s, 2], at(-1, dc)))
    for c in edges:
        c.start()
    settle(1)
    ext[SHIFT : SHIFT + rows, SHIFT : SHIFT + cols, :] = x1[...].astype(f32)
    for k in range(cols // chunk0):
        for c in halo(k):
            c.wait()
    for c in edges:
        c.wait()
    ext[:SHIFT, SHIFT : SHIFT + cols, :] = top[...].astype(f32)
    ext[SHIFT + rows :, SHIFT : SHIFT + cols, :] = bot[...].astype(f32)
    for s in range(2):
        take = slice(edge - SHIFT, edge) if s == 0 else slice(0, SHIFT)
        put = slice(0, SHIFT) if s == 0 else slice(SHIFT + cols, 2 * SHIFT + cols)
        ext[SHIFT : SHIFT + rows, put, :] = side[s].astype(f32)[:, take, :]
        ext[:SHIFT, put, :] = corner[s, 0].astype(f32)[:, take, :]
        ext[SHIFT + rows :, put, :] = corner[s, 1].astype(f32)[:, take, :]
    half = WIN // 2

    def shifted(k, _):
        span = pl.ds(pl.multiple_of(k * chunk1, WIN), chunk1)
        y = second_chunk(ext[:, span, :], regb[:, span, :], w, heads, hmask).astype(f32)
        m = half * WIN
        g = chunk1 // WIN
        for r in range(2):
            for q in range(g):
                e = (r * g + q) * m
                place = pl.ds(pl.multiple_of(k * chunk1 + q * WIN, WIN), WIN)
                res[r * half : (r + 1) * half, place, :] = y[e : e + m].reshape(half, WIN, width)
        return 0

    lax.fori_loop(0, (cols + 2 * SHIFT) // chunk1, shifted, 0)
    o_ref[...] = res[:, SHIFT : SHIFT + cols, :].astype(bf16)
    for c in list(direct.values()) + list(relays.values()):
        c.wait_send()


def chunk_of(windows, most):
    return max(d for d in range(1, most + 1) if windows % d == 0) * WIN


def on_device(*args):
    x, labels, rel_index = args[:3]
    qkv_weight, qkv_bias, bias_table, proj_weight = args[5:9]
    fc1_weight, fc1_bias, fc2_weight = args[10:13]
    rows, cols, width = x.shape
    n = lax.axis_size("ch")
    heads = bias_table.shape[2] * n
    hidden = fc1_weight.shape[2] * n
    chunk0, chunk1 = chunk_of(cols // WIN, 8), chunk_of(cols // WIN + 1, 11)
    tall, wide = rows + 2 * SHIFT, cols + 2 * SHIFT
    edge, keys = 16, WIN * WIN
    dma = pltpu.SemaphoreType.DMA
    vm = pltpu.VMEM
    entries = bias_table.shape[1] + -bias_table.shape[1] % 128
    scratch = [
        vm((tall, wide, width), f32), vm((tall, wide, 128), f32), vm((rows, wide, width), f32),
        vm((rows, cols, width), bf16), vm((SHIFT, cols, width), bf16), vm((SHIFT, cols, width), bf16),
        vm((2, rows, edge, width), bf16), vm((2, 2, SHIFT, edge, width), bf16), vm((8, rows, cols), jnp.int32),
        vm((entries, 128), f32), vm((BLOCKS, 8, entries), f32), vm((n, BLOCKS, 8, entries), f32),
        vm((n,) + qkv_weight.shape, bf16), vm((n,) + qkv_bias.shape, f32), vm((n,) + fc1_bias.shape, f32),
        vm((BLOCKS, width, 3 * width), bf16), vm((BLOCKS, 1, 3 * width), f32),
        vm((BLOCKS, keys, heads * keys), f32), vm((BLOCKS, width, width), bf16),
        vm((BLOCKS, width, hidden), bf16), vm((BLOCKS, 1, hidden), f32), vm((BLOCKS, hidden, width), bf16),
        dma((n - 1, BLOCKS + 1, 4)), dma((n - 1, BLOCKS + 1, 4)),
        dma((n - 1, BLOCKS, 4)), dma((n - 1, BLOCKS, 4)),
        dma((8,)), dma((8,)), dma((2, cols // chunk0)), dma((2, cols // chunk0)), dma((2, 3)), dma((2, 3)),
        dma((7,)),
    ]
    vmem = pl.BlockSpec(memory_space=vm)
    return pl.pallas_call(
        functools.partial(fused, heads, chunk0, chunk1),
        out_shape=jax.ShapeDtypeStruct(x.shape, bf16),
        in_specs=[vmem] * len(args),
        out_specs=vmem,
        scratch_shapes=scratch,
        compiler_params=pltpu.CompilerParams(
            collective_id=0, has_side_effects=True, vmem_limit_bytes=60 * 1024 * 1024
        ),
        name="fused",
    )(*args)


def solution(mesh):
    in_specs = (
        P(("row", "ch"), "col", None), P(("row", "ch"), "col"), P(), P(), P(),
        P(None, None, None, "ch"), P(None, None, "ch"), P(None, None, "ch"), P(None, "ch", None), P(),
        P(None, None, "ch"), P(None, "ch"), P(None, "ch", None), P(),
    )
    out_specs = P(("row", "ch"), "col", None)
    return jax.shard_map(on_device, mesh=mesh, in_specs=in_specs, out_specs=out_specs, check_vma=False)
```

```python
import functools

import jax
import jax.numpy as jnp
from jax import lax
from jax.experimental import pallas as pl
from jax.experimental.pallas import tpu as pltpu
from jax.sharding import PartitionSpec as P

WIN = 8
SHIFT = 4
BLOCKS = 2
EPS = 1e-05
FAR = -1e30
LOG2E = 1.4426950408889634
GROUP = 4
bf16 = jnp.bfloat16
f32 = jnp.float32


def dot(a, b):
    return jnp.dot(a, b, preferred_element_type=f32)


def dot_t(a, b):
    return lax.dot_general(a, b, (((1,), (1,)), ((), ())), preferred_element_type=f32)


def layer_norm(x, gain, offset):
    center = x - jnp.mean(x, axis=-1, keepdims=True)
    spread = jnp.mean(center * center, axis=-1, keepdims=True)
    return (center * lax.rsqrt(spread + EPS) * gain + offset).astype(bf16)


def rows_of(x):
    return x.reshape(x.shape[0] * x.shape[1], x.shape[2])


def attend(group, hmask, bias, heads, depth):
    keys, width = group[0][1].shape
    per = 128 // keys
    scores, values = [], []
    for q, k, v, far in group:
        kb = jnp.concatenate([k] * heads, axis=0) * hmask
        if far is not None:
            q = jnp.concatenate([q, far[0]], axis=1)
            kb = jnp.concatenate([kb, jnp.concatenate([far[1]] * heads, axis=0)], axis=1)
        scores.append(dot_t(q, kb))
        values.append(jnp.concatenate([jnp.concatenate([v] * heads, axis=0) * hmask, hmask], axis=1))
    lane = lax.broadcasted_iota(jnp.int32, (scores[0].shape[0], 128), 1)
    weights = []
    for s in scores:
        s = s * (depth ** (-0.5) * LOG2E) + bias
        parts = []
        for c in range(0, s.shape[1], 128):
            t = s[:, c : c + 128]
            top = None
            for j in range(per):
                inside = (lane >= j * keys) & (lane < (j + 1) * keys)
                peak = jnp.max(jnp.where(inside, t, -jnp.inf), axis=-1, keepdims=True)
                top = peak if top is None else jnp.where(lane >= j * keys, peak, top)
            parts.append(jnp.exp2(t - top))
        weights.append(jnp.concatenate(parts, axis=1).astype(bf16))
    outs = [dot(p, v) for p, v in zip(weights, values)]
    return [(o[:, :width] / o[:, width:]).astype(bf16) for o in outs]


def finish(x, attended, w, b):
    mixed = dot(attended, w["proj"][b])
    middle = (x + mixed + w["proj_b"][b]).astype(bf16).astype(f32)
    normed = layer_norm(middle, w["gain"][b][1:2], w["shift"][b][1:2])
    inner = dot(normed, w["fc1"][b]) + w["fc1_b"][b]
    hidden = (0.5 * inner * (1.0 + lax.erf(inner * (0.5 ** 0.5)))).astype(bf16)
    outer = dot(hidden, w["fc2"][b])
    return (middle + outer + w["fc2_b"][b]).astype(bf16)


def head_mask(heads, keys, width):
    depth = width // heads
    row = lax.broadcasted_iota(jnp.int32, (heads * keys, width), 0) // keys
    col = lax.broadcasted_iota(jnp.int32, (heads * keys, width), 1) // depth
    return (row == col).astype(f32).astype(bf16)


def qkv_of(x, w, b):
    normed = layer_norm(x, w["gain"][b][0:1], w["shift"][b][0:1])
    return dot_t(normed, rows_of(w["qkv"][b])) + w["qkv_b"][b]


def first_chunk(x, w, heads, hmask):
    rows, wide, width = x.shape
    depth = width // heads
    toks = jnp.concatenate(
        [rows_of(x[:, c : c + WIN]) for c in range(0, wide, WIN)], axis=0
    )
    triple = qkv_of(toks, w, 0)
    outs = []
    n = WIN * WIN
    windows = []
    for g in range(wide // WIN):
        t = triple[g * n : (g + 1) * n].astype(bf16)
        windows.append((t[:, :width], t[:, width : 2 * width], t[:, 2 * width :], None))
    for g in range(0, len(windows), GROUP):
        outs += attend(windows[g : g + GROUP], hmask, w["bias"][0], heads, depth)
    return finish(toks, jnp.concatenate(outs, axis=0), w, 0)


def second_chunk(x, reg, w, heads, hmask):
    kinds = lax.broadcasted_iota(jnp.int32, (WIN * WIN, 128), 1).astype(f32)
    rows, wide, width = x.shape
    depth = width // heads
    half = WIN // 2
    outs, toks = [], []
    n = WIN * WIN
    for r in range(0, rows, WIN):
        xs = [rows_of(x[r : r + WIN, c : c + WIN]) for c in range(0, wide, WIN)]
        same = [(rows_of(reg[r : r + WIN, c : c + WIN]) == kinds).astype(f32) for c in range(0, wide, WIN)]
        triple = qkv_of(jnp.concatenate(xs, axis=0), w, 1)
        own = slice(half * WIN, n) if r == 0 else slice(0, half * WIN)
        bias = w["bias"][1][own, :]
        windows = []
        for g in range(wide // WIN):
            t = triple[g * n : (g + 1) * n].astype(bf16)
            far = (same[g][own] * FAR).astype(bf16), (1.0 - same[g]).astype(bf16)
            windows.append((t[own, :width], t[:, width : 2 * width], t[:, 2 * width :], far))
            toks.append(xs[g][own])
        for g in range(0, len(windows), GROUP):
            outs += attend(windows[g : g + GROUP], hmask, bias, heads, depth)
    return finish(jnp.concatenate(toks, axis=0), jnp.concatenate(outs, axis=0), w, 1)


def fused(
    heads, chunk0, chunk1,
    x_ref, lab_ref, rel_ref, gain, shift, qkv_w, qkv_b, table, proj_w, proj_b, fc1_w, fc1_b, fc2_w, fc2_b,
    o_ref,
    ext, regb, res, x1, top, bot, side, corner, lab, tab_own, tab_all,
    qb_all, f1b_all, qkv, qb, bias, proj, fc1, f1b, fc2,
    wsend, wrecv, rsend, rrecv, lsend, lrecv, hsend, hrecv, esend, erecv, own_sem,
):
    rows, cols, width = x_ref.shape
    n = lax.axis_size("ch")
    nrow, ncol = lax.axis_size("row"), lax.axis_size("col")
    row, col, ch = lax.axis_index("row"), lax.axis_index("col"), lax.axis_index("ch")
    ring = row * n + ch
    total = nrow * n

    def at(dr, dc):
        p = lax.rem(ring + dr + total, total)
        return (p // n, lax.rem(col + dc + ncol, ncol), lax.rem(p, n))

    around = [(-1, -1), (-1, 0), (-1, 1), (0, -1), (0, 1), (1, -1), (1, 0), (1, 1)]
    peers = [(row, col, lax.rem(ch + d, n)) for d in range(1, n)]
    mate = (row, col + 1 - 2 * lax.rem(col, 2), ch)
    core = lax.rem(col, 2)
    mesh_id = pl.DeviceIdType.MESH

    barrier = pltpu.get_barrier_semaphore()
    targets = [at(*d) for d in around] + peers + [mate]
    for t in targets:
        pl.semaphore_signal(barrier, inc=1, device_id=t, device_id_type=mesh_id)

    def remote(src, dst, ssem, rsem, to):
        return pltpu.make_async_remote_copy(
            src_ref=src, dst_ref=dst, send_sem=ssem, recv_sem=rsem, device_id=to, device_id_type=mesh_id
        )

    tab_own[...] = jnp.zeros_like(tab_own)
    tab_own[:, : table.shape[1], : table.shape[2]] = table[...]
    pl.semaphore_wait(barrier, len(targets))

    part = width // n
    kh, ph, fh, gh = qkv_w.shape[2] // 2, proj_w.shape[1] // 2, width // 2, fc2_w.shape[1] // 2
    pw, fw, gw = proj_w.shape[1], fc1_w.shape[2], fc2_w.shape[1]

    def pieces(b, owner):
        k0, p0, f0, g0 = (pl.multiple_of(core * v, 16) for v in (kh, ph, fh, gh))
        return [
            (qkv_w.at[b, :, pl.ds(k0, kh), :], qkv.at[b, :, pl.ds(pl.multiple_of(owner * part + k0, 16), kh), :]),
            (proj_w.at[b, pl.ds(p0, ph), :], proj.at[b, pl.ds(pl.multiple_of(owner * pw + p0, 16), ph), :]),
            (
                fc1_w.at[b, pl.ds(f0, fh), :],
                fc1.at[b, pl.ds(f0, fh), pl.ds(pl.multiple_of(owner * fw, 128), fw)],
            ),
            (fc2_w.at[b, pl.ds(g0, gh), :], fc2.at[b, pl.ds(pl.multiple_of(owner * gw + g0, 16), gh), :]),
        ]

    direct, relays, smalls = {}, {}, []
    for d in range(1, n):
        to, owner = peers[d - 1], lax.rem(ch - d + n, n)
        for b in range(BLOCKS):
            for i, (src, dst) in enumerate(pieces(b, ch)):
                direct[d, b, i] = remote(src, dst, wsend.at[d - 1, b, i], wrecv.at[d - 1, b, i], to)
            for i, (_, dst) in enumerate(pieces(b, owner)):
                relays[d, b, i] = remote(dst, dst, rsend.at[d - 1, b, i], rrecv.at[d - 1, b, i], mate)
        for i, (src, dst) in enumerate(
            [(tab_own, tab_all.at[ch]), (qkv_b, qb_all.at[ch]), (fc1_b, f1b_all.at[ch])]
        ):
            smalls.append(remote(src, dst, wsend.at[d - 1, BLOCKS, i], wrecv.at[d - 1, BLOCKS, i], to))
    for c in smalls:
        c.start()
    for d in range(1, n):
        for i in range(4):
            direct[d, 0, i].start()
    labels = []
    for i, d in enumerate(around):
        labels.append(remote(lab_ref, lab.at[i], lsend.at[i], lrecv.at[i], at(-d[0], -d[1])))
        labels[-1].start()
    for d in range(1, n):
        for i in range(4):
            direct[d, 1, i].start()
    locals_ = [
        (qkv_w, qkv.at[:, :, pl.ds(pl.multiple_of(ch * part, 16), part), :]),
        (proj_w, proj.at[:, pl.ds(pl.multiple_of(ch * pw, 16), pw), :]),
        (fc1_w, fc1.at[:, :, pl.ds(pl.multiple_of(ch * fw, 128), fw)]),
        (fc2_w, fc2.at[:, pl.ds(pl.multiple_of(ch * gw, 16), gw), :]),
        (tab_own, tab_all.at[ch]), (qkv_b, qb_all.at[ch]), (fc1_b, f1b_all.at[ch]),
    ]
    locals_ = [pltpu.make_async_copy(s, d, own_sem.at[i]) for i, (s, d) in enumerate(locals_)]
    for c in locals_:
        c.start()
    for c in locals_:
        c.wait()
    for c in smalls:
        c.wait()

    keys = WIN * WIN
    for j in range(n):
        for b in range(BLOCKS):
            for m in range(3):
                qb[b, :, m * width + j * part : m * width + (j + 1) * part] = qb_all[j, m, b : b + 1, :]
            f1b[b, :, j * fw : (j + 1) * fw] = f1b_all[j, b : b + 1, :]
    local_heads = table.shape[1]
    per = 128 // keys
    idx = jnp.concatenate([rel_ref[...]] * per, axis=1)
    lane = lax.broadcasted_iota(jnp.int32, idx.shape, 1)
    for b in range(BLOCKS):
        for t in range(heads // per):
            out = None
            for j in range(per):
                h = t * per + j
                entry = tab_all[h // local_heads, b, h % local_heads : h % local_heads + 1, :]
                got = None
                for c in range(0, entry.shape[1], 128):
                    piece = jnp.broadcast_to(entry[:, c : c + 128], idx.shape)
                    here = jnp.take_along_axis(piece, idx & 127, axis=1, mode="promise_in_bounds")
                    got = here if got is None else jnp.where(idx >= c, here, got)
                out = got if out is None else jnp.where(lane >= j * keys, got, out)
            bias[b, :, t * 128 : (t + 1) * 128] = out * LOG2E

    def bring(b):
        for d in range(1, n):
            for i in range(4):
                direct[d, b, i].wait_recv()
                relays[d, b, i].start()

    def settle(b):
        for d in range(1, n):
            for i in range(4):
                relays[d, b, i].wait_recv()

    bring(0)
    settle(0)
    w = {
        "gain": gain, "shift": shift, "qkv": qkv, "qkv_b": qb, "bias": bias, "proj": proj,
        "proj_b": [proj_b[b : b + 1] for b in range(BLOCKS)], "fc1": fc1, "fc1_b": f1b, "fc2": fc2,
        "fc2_b": [fc2_b[b : b + 1] for b in range(BLOCKS)],
    }
    hmask = head_mask(heads, keys, width)

    def halo(k):
        span = pl.ds(pl.multiple_of(k * chunk0, chunk0), chunk0)
        return [
            remote(x1.at[rows - SHIFT :, span, :], top.at[:, span, :], hsend.at[0, k], hrecv.at[0, k], at(1, 0)),
            remote(x1.at[:SHIFT, span, :], bot.at[:, span, :], hsend.at[1, k], hrecv.at[1, k], at(-1, 0)),
        ]

    def regular(step, _):
        k = lax.rem(step + 1, cols // chunk0)
        span = pl.ds(pl.multiple_of(k * chunk0, chunk0), chunk0)
        y = first_chunk(x_ref[:, span, :].astype(f32), w, heads, hmask).astype(f32)
        m = WIN * WIN
        y = jnp.concatenate(
            [y[g * m : (g + 1) * m].reshape(WIN, WIN, width) for g in range(chunk0 // WIN)], axis=1
        )
        x1[:, span, :] = y.astype(bf16)
        for c in halo(k):
            c.start()
        return 0

    lax.fori_loop(0, cols // chunk0, regular, 0)
    edge = side.shape[2]
    edges = []
    for s, dc in ((0, 1), (1, -1)):
        span = slice(cols - edge, cols) if dc == 1 else slice(0, edge)
        edges.append(remote(x1.at[:, span, :], side.at[s], esend.at[s, 0], erecv.at[s, 0], at(0, dc)))
        edges.append(
            remote(x1.at[rows - SHIFT :, span, :], corner.at[s, 0], esend.at[s, 1], erecv.at[s, 1], at(1, dc))
        )
        edges.append(remote(x1.at[:SHIFT, span, :], corner.at[s, 1], esend.at[s, 2], erecv.at[s, 2], at(-1, dc)))
    for c in edges:
        c.start()
    bring(1)
    for c in labels:
        c.wait()
    def column(up, mid, down):
        return jnp.concatenate([up[rows - SHIFT :], mid, down[:SHIFT]], axis=0)
    west = column(lab[0], lab[3], lab[5]).astype(f32)
    mid = column(lab[1], lab_ref[...], lab[6]).astype(f32)
    east = column(lab[2], lab[4], lab[7]).astype(f32)
    tall = rows + 2 * SHIFT
    moved = pltpu.roll(jnp.concatenate([mid, jnp.zeros((tall, 128), f32)], axis=1), SHIFT, 1)
    span = cols + 128
    j = lax.broadcasted_iota(jnp.int32, (tall, span), 1)
    i = lax.broadcasted_iota(jnp.int32, (tall, span), 0)
    blank = jnp.zeros((tall, span - 128), f32)
    left = jnp.concatenate([pltpu.roll(west[:, cols - 128 :], SHIFT, 1), blank], axis=1)
    right = jnp.concatenate([blank, pltpu.roll(east[:, :128], SHIFT, 1)], axis=1)
    kind = jnp.where(j < SHIFT, left, jnp.where(j < cols + SHIFT, moved, right))
    def flag(here, when):
        return jnp.where(here, when.astype(f32), 0.0)
    low = flag((i >= SHIFT) & (i < 2 * SHIFT), ring == 0) + flag(i >= rows + SHIFT, ring == total - 1)
    front = flag((j >= SHIFT) & (j < 2 * SHIFT), col == 0) + flag(j >= cols + SHIFT, col == ncol - 1)
    kind = kind * 4.0 + low * 2.0 + front
    turned = kind.T[: cols + 2 * SHIFT].astype(bf16)
    pick = lax.broadcasted_iota(jnp.int32, (tall, 128), 0)
    for r in range(tall):
        regb[r] = dot(turned, (pick == r).astype(f32).astype(bf16))
    settle(1)
    ext[SHIFT : SHIFT + rows, SHIFT : SHIFT + cols, :] = x1[...].astype(f32)
    def land(k):
        span = slice(k * chunk0, (k + 1) * chunk0)
        put = slice(SHIFT + k * chunk0, SHIFT + (k + 1) * chunk0)
        for c in halo(k):
            c.wait()
        ext[:SHIFT, put, :] = top[:, span, :].astype(f32)
        ext[SHIFT + rows :, put, :] = bot[:, span, :].astype(f32)

    half = WIN // 2

    def shifted(k, _):
        span = pl.ds(pl.multiple_of(k * chunk1, WIN), chunk1)
        y = second_chunk(ext[:, span, :], regb[:, span, :], w, heads, hmask).astype(f32)
        m = half * WIN
        g = chunk1 // WIN
        for r in range(2):
            for q in range(g):
                e = (r * g + q) * m
                place = pl.ds(pl.multiple_of(k * chunk1 + q * WIN, WIN), WIN)
                res[r * half : (r + 1) * half, place, :] = y[e : e + m].reshape(half, WIN, width)
        return 0

    steps = (cols + 2 * SHIFT) // chunk1
    first, last = (chunk1 - SHIFT) // chunk0, ((steps - 1) * chunk1 - SHIFT - 1) // chunk0
    ready = range(first, last + 1) if steps > 2 else ()
    for k in ready:
        land(k)
    if steps > 2:
        lax.fori_loop(1, steps - 1, shifted, 0)
    for k in range(cols // chunk0):
        if k not in ready:
            land(k)
    for c in edges:
        c.wait()
    for s in range(2):
        take = slice(edge - SHIFT, edge) if s == 0 else slice(0, SHIFT)
        put = slice(0, SHIFT) if s == 0 else slice(SHIFT + cols, 2 * SHIFT + cols)
        ext[SHIFT : SHIFT + rows, put, :] = side[s].astype(f32)[:, take, :]
        ext[:SHIFT, put, :] = corner[s, 0].astype(f32)[:, take, :]
        ext[SHIFT + rows :, put, :] = corner[s, 1].astype(f32)[:, take, :]
    if steps > 1:
        lax.fori_loop(0, 2, lambda i, c: shifted(i * (steps - 1), c), 0)
    else:
        shifted(0, 0)
    o_ref[...] = res[:, SHIFT : SHIFT + cols, :].astype(bf16)
    for c in list(direct.values()) + list(relays.values()):
        c.wait_send()


def chunk_of(windows, most):
    return max(d for d in range(1, most + 1) if windows % d == 0) * WIN


def on_device(*args):
    x, labels, rel_index = args[:3]
    qkv_weight, qkv_bias, bias_table, proj_weight = args[5:9]
    fc1_weight, fc1_bias, fc2_weight = args[10:13]
    rows, cols, width = x.shape
    n = lax.axis_size("ch")
    heads = bias_table.shape[2] * n
    args = list(args)
    args[5] = qkv_weight.swapaxes(2, 3)
    args[6] = qkv_bias.swapaxes(0, 1)
    args[7] = bias_table.swapaxes(1, 2)
    hidden = fc1_weight.shape[2] * n
    chunk0, chunk1 = chunk_of(cols // WIN, 8), chunk_of(cols // WIN + 1, 11)
    tall, wide = rows + 2 * SHIFT, cols + 2 * SHIFT
    edge, keys = 16, WIN * WIN
    dma = pltpu.SemaphoreType.DMA
    vm = pltpu.VMEM
    entries = bias_table.shape[1] + -bias_table.shape[1] % 128
    scratch = [
        vm((tall, wide, width), f32), vm((tall, wide, 128), f32), vm((rows, wide, width), f32),
        vm((rows, cols, width), bf16), vm((SHIFT, cols, width), bf16), vm((SHIFT, cols, width), bf16),
        vm((2, rows, edge, width), bf16), vm((2, 2, SHIFT, edge, width), bf16), vm((8, rows, cols), jnp.int32),
        vm((BLOCKS, 8, entries), f32), vm((n, BLOCKS, 8, entries), f32),
        vm((n,) + args[6].shape, f32), vm((n,) + fc1_bias.shape, f32),
        vm((BLOCKS, 3, width, width), bf16), vm((BLOCKS, 1, 3 * width), f32),
        vm((BLOCKS, keys, heads * keys), f32), vm((BLOCKS, width, width), bf16),
        vm((BLOCKS, width, hidden), bf16), vm((BLOCKS, 1, hidden), f32), vm((BLOCKS, hidden, width), bf16),
        dma((n - 1, BLOCKS + 1, 4)), dma((n - 1, BLOCKS + 1, 4)),
        dma((n - 1, BLOCKS, 4)), dma((n - 1, BLOCKS, 4)),
        dma((8,)), dma((8,)), dma((2, cols // chunk0)), dma((2, cols // chunk0)), dma((2, 3)), dma((2, 3)),
        dma((7,)),
    ]
    vmem = pl.BlockSpec(memory_space=vm)
    return pl.pallas_call(
        functools.partial(fused, heads, chunk0, chunk1),
        out_shape=jax.ShapeDtypeStruct(x.shape, bf16),
        in_specs=[vmem] * len(args),
        out_specs=vmem,
        scratch_shapes=scratch,
        compiler_params=pltpu.CompilerParams(
            collective_id=0, has_side_effects=True, vmem_limit_bytes=60 * 1024 * 1024
        ),
        name="fused",
    )(*args)


def solution(mesh):
    in_specs = (
        P(("row", "ch"), "col", None), P(("row", "ch"), "col"), P(), P(), P(),
        P(None, None, None, "ch"), P(None, None, "ch"), P(None, None, "ch"), P(None, "ch", None), P(),
        P(None, None, "ch"), P(None, "ch"), P(None, "ch", None), P(),
    )
    out_specs = P(("row", "ch"), "col", None)
    return jax.shard_map(on_device, mesh=mesh, in_specs=in_specs, out_specs=out_specs, check_vma=False)
```

```python
import functools

import jax
import jax.numpy as jnp
from jax import lax
from jax.experimental import pallas as pl
from jax.experimental.pallas import tpu as pltpu
from jax.sharding import PartitionSpec as P

WIN = 8
SHIFT = 4
BLOCKS = 2
EPS = 1e-05
FAR = -1e30
LOG2E = 1.4426950408889634
GROUP = 22
bf16 = jnp.bfloat16
f32 = jnp.float32


def dot(a, b):
    return jnp.dot(a, b, preferred_element_type=f32)


def dot_t(a, b):
    return lax.dot_general(a, b, (((1,), (1,)), ((), ())), preferred_element_type=f32)


def layer_norm(x, gain, offset):
    center = x - jnp.mean(x, axis=-1, keepdims=True)
    spread = jnp.mean(center * center, axis=-1, keepdims=True)
    return (center * lax.rsqrt(spread + EPS) * gain + offset).astype(bf16)


def rows_of(x):
    return x.reshape(x.shape[0] * x.shape[1], x.shape[2])


def attend(group, hmask, heads, depth):
    keys, width = group[0][1].shape
    per = 128 // keys
    scores, values = [], []
    for q, k, v, far, _ in group:
        kb = jnp.concatenate([k] * heads, axis=0) * hmask
        if far is not None:
            q = jnp.concatenate([q, far[0]], axis=1)
            kb = jnp.concatenate([kb, jnp.concatenate([far[1]] * heads, axis=0)], axis=1)
        scores.append(dot_t(q, kb))
        values.append(jnp.concatenate([jnp.concatenate([v] * heads, axis=0) * hmask, hmask], axis=1))
    lane = lax.broadcasted_iota(jnp.int32, (scores[0].shape[0], 128), 1)
    weights = []
    for s, (_, _, _, _, bias) in zip(scores, group):
        s = s * (depth ** (-0.5) * LOG2E) + bias
        parts = []
        for c in range(0, s.shape[1], 128):
            t = s[:, c : c + 128]
            top = None
            for j in range(per):
                inside = (lane >= j * keys) & (lane < (j + 1) * keys)
                peak = jnp.max(jnp.where(inside, t, -jnp.inf), axis=-1, keepdims=True)
                top = peak if top is None else jnp.where(lane >= j * keys, peak, top)
            parts.append(jnp.exp2(t - top))
        weights.append(jnp.concatenate(parts, axis=1).astype(bf16))
    outs = [dot(p, v) for p, v in zip(weights, values)]
    return [(o[:, :width] / o[:, width:]).astype(bf16) for o in outs]


def finish(x, attended, w, b):
    mixed = dot(attended, w["proj"][b])
    middle = (x + mixed + w["proj_b"][b]).astype(bf16).astype(f32)
    normed = layer_norm(middle, w["gain"][b][1:2], w["shift"][b][1:2])
    inner = dot(normed, w["fc1"][b]) + w["fc1_b"][b]
    hidden = (0.5 * inner * (1.0 + lax.erf(inner * (0.5 ** 0.5)))).astype(bf16)
    outer = dot(hidden, w["fc2"][b])
    return (middle + outer + w["fc2_b"][b]).astype(bf16)


def head_mask(heads, keys, width):
    depth = width // heads
    row = lax.broadcasted_iota(jnp.int32, (heads * keys, width), 0) // keys
    col = lax.broadcasted_iota(jnp.int32, (heads * keys, width), 1) // depth
    return (row == col).astype(f32).astype(bf16)


def qkv_of(x, w, b):
    normed = layer_norm(x, w["gain"][b][0:1], w["shift"][b][0:1])
    return dot_t(normed, rows_of(w["qkv"][b])) + w["qkv_b"][b]


def first_chunk(x, w, heads, hmask):
    rows, wide, width = x.shape
    depth = width // heads
    toks = jnp.concatenate(
        [rows_of(x[:, c : c + WIN]) for c in range(0, wide, WIN)], axis=0
    )
    triple = qkv_of(toks, w, 0)
    outs = []
    n = WIN * WIN
    windows = []
    for g in range(wide // WIN):
        t = triple[g * n : (g + 1) * n].astype(bf16)
        windows.append((t[:, :width], t[:, width : 2 * width], t[:, 2 * width :], None, w["bias"][0]))
    for g in range(0, len(windows), GROUP):
        outs += attend(windows[g : g + GROUP], hmask, heads, depth)
    return finish(toks, jnp.concatenate(outs, axis=0), w, 0)


def second_chunk(x, reg, w, heads, hmask):
    kinds = lax.broadcasted_iota(jnp.int32, (WIN * WIN, 128), 1).astype(f32)
    rows, wide, width = x.shape
    depth = width // heads
    half = WIN // 2
    outs, toks, windows = [], [], []
    n = WIN * WIN
    for r in range(0, rows, WIN):
        xs = [rows_of(x[r : r + WIN, c : c + WIN]) for c in range(0, wide, WIN)]
        same = [(rows_of(reg[r : r + WIN, c : c + WIN]) == kinds).astype(f32) for c in range(0, wide, WIN)]
        triple = qkv_of(jnp.concatenate(xs, axis=0), w, 1)
        own = slice(half * WIN, n) if r == 0 else slice(0, half * WIN)
        bias = w["bias"][1][own, :]
        for g in range(wide // WIN):
            t = triple[g * n : (g + 1) * n].astype(bf16)
            far = (same[g][own] * FAR).astype(bf16), (1.0 - same[g]).astype(bf16)
            windows.append((t[own, :width], t[:, width : 2 * width], t[:, 2 * width :], far, bias))
            toks.append(xs[g][own])
    for g in range(0, len(windows), GROUP):
        outs += attend(windows[g : g + GROUP], hmask, heads, depth)
    return finish(jnp.concatenate(toks, axis=0), jnp.concatenate(outs, axis=0), w, 1)


def fused(
    heads, chunk0, chunk1,
    x_ref, lab_ref, rel_ref, gain, shift, qkv_w, qkv_b, table, proj_w, proj_b, fc1_w, fc1_b, fc2_w, fc2_b,
    o_ref,
    ext, regb, res, x1, top, bot, side, corner, lab, tab_own, tab_all,
    qb_all, f1b_all, qkv, qb, bias, proj, fc1, f1b, fc2,
    wsend, wrecv, rsend, rrecv, lsend, lrecv, hsend, hrecv, esend, erecv, own_sem,
):
    rows, cols, width = x_ref.shape
    n = lax.axis_size("ch")
    nrow, ncol = lax.axis_size("row"), lax.axis_size("col")
    row, col, ch = lax.axis_index("row"), lax.axis_index("col"), lax.axis_index("ch")
    ring = row * n + ch
    total = nrow * n

    def at(dr, dc):
        p = lax.rem(ring + dr + total, total)
        return (p // n, lax.rem(col + dc + ncol, ncol), lax.rem(p, n))

    around = [(-1, -1), (-1, 0), (-1, 1), (0, -1), (0, 1), (1, -1), (1, 0), (1, 1)]
    peers = [(row, col, lax.rem(ch + d, n)) for d in range(1, n)]
    mate = (row, col + 1 - 2 * lax.rem(col, 2), ch)
    core = lax.rem(col, 2)
    mesh_id = pl.DeviceIdType.MESH

    barrier = pltpu.get_barrier_semaphore()
    targets = [at(*d) for d in around] + peers + [mate]
    for t in targets:
        pl.semaphore_signal(barrier, inc=1, device_id=t, device_id_type=mesh_id)

    def remote(src, dst, ssem, rsem, to):
        return pltpu.make_async_remote_copy(
            src_ref=src, dst_ref=dst, send_sem=ssem, recv_sem=rsem, device_id=to, device_id_type=mesh_id
        )

    tab_own[...] = jnp.zeros_like(tab_own)
    tab_own[:, : table.shape[1], : table.shape[2]] = table[...]
    pl.semaphore_wait(barrier, len(targets))

    part = width // n
    kh, ph, fh, gh = qkv_w.shape[2] // 2, proj_w.shape[1] // 2, width // 2, fc2_w.shape[1] // 2
    pw, fw, gw = proj_w.shape[1], fc1_w.shape[2], fc2_w.shape[1]

    def pieces(b, owner):
        k0, p0, f0, g0 = (pl.multiple_of(core * v, 16) for v in (kh, ph, fh, gh))
        return [
            (qkv_w.at[b, :, pl.ds(k0, kh), :], qkv.at[b, :, pl.ds(pl.multiple_of(owner * part + k0, 16), kh), :]),
            (proj_w.at[b, pl.ds(p0, ph), :], proj.at[b, pl.ds(pl.multiple_of(owner * pw + p0, 16), ph), :]),
            (
                fc1_w.at[b, pl.ds(f0, fh), :],
                fc1.at[b, pl.ds(f0, fh), pl.ds(pl.multiple_of(owner * fw, 128), fw)],
            ),
            (fc2_w.at[b, pl.ds(g0, gh), :], fc2.at[b, pl.ds(pl.multiple_of(owner * gw + g0, 16), gh), :]),
        ]

    direct, relays, smalls = {}, {}, []
    for d in range(1, n):
        to, owner = peers[d - 1], lax.rem(ch - d + n, n)
        for b in range(BLOCKS):
            for i, (src, dst) in enumerate(pieces(b, ch)):
                direct[d, b, i] = remote(src, dst, wsend.at[d - 1, b, i], wrecv.at[d - 1, b, i], to)
            for i, (_, dst) in enumerate(pieces(b, owner)):
                relays[d, b, i] = remote(dst, dst, rsend.at[d - 1, b, i], rrecv.at[d - 1, b, i], mate)
        for i, (src, dst) in enumerate(
            [(tab_own, tab_all.at[ch]), (qkv_b, qb_all.at[ch]), (fc1_b, f1b_all.at[ch])]
        ):
            smalls.append(remote(src, dst, wsend.at[d - 1, BLOCKS, i], wrecv.at[d - 1, BLOCKS, i], to))
    for c in smalls:
        c.start()
    for d in range(1, n):
        for i in range(4):
            direct[d, 0, i].start()
    labels = []
    for i, d in enumerate(around):
        labels.append(remote(lab_ref, lab.at[i], lsend.at[i], lrecv.at[i], at(-d[0], -d[1])))
        labels[-1].start()
    for d in range(1, n):
        for i in range(4):
            direct[d, 1, i].start()
    locals_ = [
        (qkv_w, qkv.at[:, :, pl.ds(pl.multiple_of(ch * part, 16), part), :]),
        (proj_w, proj.at[:, pl.ds(pl.multiple_of(ch * pw, 16), pw), :]),
        (fc1_w, fc1.at[:, :, pl.ds(pl.multiple_of(ch * fw, 128), fw)]),
        (fc2_w, fc2.at[:, pl.ds(pl.multiple_of(ch * gw, 16), gw), :]),
        (tab_own, tab_all.at[ch]), (qkv_b, qb_all.at[ch]), (fc1_b, f1b_all.at[ch]),
    ]
    locals_ = [pltpu.make_async_copy(s, d, own_sem.at[i]) for i, (s, d) in enumerate(locals_)]
    for c in locals_:
        c.start()
    for c in locals_:
        c.wait()
    for c in smalls:
        c.wait()

    keys = WIN * WIN
    for j in range(n):
        for b in range(BLOCKS):
            for m in range(3):
                qb[b, :, m * width + j * part : m * width + (j + 1) * part] = qb_all[j, m, b : b + 1, :]
            f1b[b, :, j * fw : (j + 1) * fw] = f1b_all[j, b : b + 1, :]
    local_heads = table.shape[1]
    per = 128 // keys
    idx = jnp.concatenate([rel_ref[...]] * per, axis=1)
    lane = lax.broadcasted_iota(jnp.int32, idx.shape, 1)
    for b in range(BLOCKS):
        for t in range(heads // per):
            out = None
            for j in range(per):
                h = t * per + j
                entry = tab_all[h // local_heads, b, h % local_heads : h % local_heads + 1, :]
                got = None
                for c in range(0, entry.shape[1], 128):
                    piece = jnp.broadcast_to(entry[:, c : c + 128], idx.shape)
                    here = jnp.take_along_axis(piece, idx & 127, axis=1, mode="promise_in_bounds")
                    got = here if got is None else jnp.where(idx >= c, here, got)
                out = got if out is None else jnp.where(lane >= j * keys, got, out)
            bias[b, :, t * 128 : (t + 1) * 128] = out * LOG2E

    def bring(b):
        for d in range(1, n):
            for i in range(4):
                direct[d, b, i].wait_recv()
                relays[d, b, i].start()

    def settle(b):
        for d in range(1, n):
            for i in range(4):
                relays[d, b, i].wait_recv()

    bring(0)
    settle(0)
    w = {
        "gain": gain, "shift": shift, "qkv": qkv, "qkv_b": qb, "bias": bias, "proj": proj,
        "proj_b": [proj_b[b : b + 1] for b in range(BLOCKS)], "fc1": fc1, "fc1_b": f1b, "fc2": fc2,
        "fc2_b": [fc2_b[b : b + 1] for b in range(BLOCKS)],
    }
    hmask = head_mask(heads, keys, width)

    def halo(k):
        span = pl.ds(pl.multiple_of(k * chunk0, chunk0), chunk0)
        return [
            remote(x1.at[rows - SHIFT :, span, :], top.at[:, span, :], hsend.at[0, k], hrecv.at[0, k], at(1, 0)),
            remote(x1.at[:SHIFT, span, :], bot.at[:, span, :], hsend.at[1, k], hrecv.at[1, k], at(-1, 0)),
        ]

    def regular(step, _):
        k = lax.rem(step + 1, cols // chunk0)
        span = pl.ds(pl.multiple_of(k * chunk0, chunk0), chunk0)
        y = first_chunk(x_ref[:, span, :].astype(f32), w, heads, hmask).astype(f32)
        m = WIN * WIN
        y = jnp.concatenate(
            [y[g * m : (g + 1) * m].reshape(WIN, WIN, width) for g in range(chunk0 // WIN)], axis=1
        )
        x1[:, span, :] = y.astype(bf16)
        for c in halo(k):
            c.start()
        return 0

    lax.fori_loop(0, cols // chunk0, regular, 0)
    edge = side.shape[2]
    edges = []
    for s, dc in ((0, 1), (1, -1)):
        span = slice(cols - edge, cols) if dc == 1 else slice(0, edge)
        edges.append(remote(x1.at[:, span, :], side.at[s], esend.at[s, 0], erecv.at[s, 0], at(0, dc)))
        edges.append(
            remote(x1.at[rows - SHIFT :, span, :], corner.at[s, 0], esend.at[s, 1], erecv.at[s, 1], at(1, dc))
        )
        edges.append(remote(x1.at[:SHIFT, span, :], corner.at[s, 1], esend.at[s, 2], erecv.at[s, 2], at(-1, dc)))
    for c in edges:
        c.start()
    bring(1)
    for c in labels:
        c.wait()
    def column(up, mid, down):
        return jnp.concatenate([up[rows - SHIFT :], mid, down[:SHIFT]], axis=0)
    west = column(lab[0], lab[3], lab[5]).astype(f32)
    mid = column(lab[1], lab_ref[...], lab[6]).astype(f32)
    east = column(lab[2], lab[4], lab[7]).astype(f32)
    tall = rows + 2 * SHIFT
    moved = pltpu.roll(jnp.concatenate([mid, jnp.zeros((tall, 128), f32)], axis=1), SHIFT, 1)
    span = cols + 128
    j = lax.broadcasted_iota(jnp.int32, (tall, span), 1)
    i = lax.broadcasted_iota(jnp.int32, (tall, span), 0)
    blank = jnp.zeros((tall, span - 128), f32)
    left = jnp.concatenate([pltpu.roll(west[:, cols - 128 :], SHIFT, 1), blank], axis=1)
    right = jnp.concatenate([blank, pltpu.roll(east[:, :128], SHIFT, 1)], axis=1)
    kind = jnp.where(j < SHIFT, left, jnp.where(j < cols + SHIFT, moved, right))
    def flag(here, when):
        return jnp.where(here, when.astype(f32), 0.0)
    low = flag((i >= SHIFT) & (i < 2 * SHIFT), ring == 0) + flag(i >= rows + SHIFT, ring == total - 1)
    front = flag((j >= SHIFT) & (j < 2 * SHIFT), col == 0) + flag(j >= cols + SHIFT, col == ncol - 1)
    kind = kind * 4.0 + low * 2.0 + front
    turned = kind.T[: cols + 2 * SHIFT].astype(bf16)
    pick = lax.broadcasted_iota(jnp.int32, (tall, 128), 0)
    for r in range(tall):
        regb[r] = dot(turned, (pick == r).astype(f32).astype(bf16))
    settle(1)
    ext[SHIFT : SHIFT + rows, SHIFT : SHIFT + cols, :] = x1[...].astype(f32)
    def land(k):
        span = slice(k * chunk0, (k + 1) * chunk0)
        put = slice(SHIFT + k * chunk0, SHIFT + (k + 1) * chunk0)
        for c in halo(k):
            c.wait()
        ext[:SHIFT, put, :] = top[:, span, :].astype(f32)
        ext[SHIFT + rows :, put, :] = bot[:, span, :].astype(f32)

    half = WIN // 2

    def shifted(k, _):
        span = pl.ds(pl.multiple_of(k * chunk1, WIN), chunk1)
        y = second_chunk(ext[:, span, :], regb[:, span, :], w, heads, hmask).astype(f32)
        m = half * WIN
        g = chunk1 // WIN
        for r in range(2):
            for q in range(g):
                e = (r * g + q) * m
                place = pl.ds(pl.multiple_of(k * chunk1 + q * WIN, WIN), WIN)
                res[r * half : (r + 1) * half, place, :] = y[e : e + m].reshape(half, WIN, width)
        return 0

    steps = (cols + 2 * SHIFT) // chunk1
    first, last = (chunk1 - SHIFT) // chunk0, ((steps - 1) * chunk1 - SHIFT - 1) // chunk0
    ready = range(first, last + 1) if steps > 2 else ()
    for k in ready:
        land(k)
    if steps > 2:
        lax.fori_loop(1, steps - 1, shifted, 0)
    for k in range(cols // chunk0):
        if k not in ready:
            land(k)
    for c in edges:
        c.wait()
    for s in range(2):
        take = slice(edge - SHIFT, edge) if s == 0 else slice(0, SHIFT)
        put = slice(0, SHIFT) if s == 0 else slice(SHIFT + cols, 2 * SHIFT + cols)
        ext[SHIFT : SHIFT + rows, put, :] = side[s].astype(f32)[:, take, :]
        ext[:SHIFT, put, :] = corner[s, 0].astype(f32)[:, take, :]
        ext[SHIFT + rows :, put, :] = corner[s, 1].astype(f32)[:, take, :]
    if steps > 1:
        lax.fori_loop(0, 2, lambda i, c: shifted(i * (steps - 1), c), 0)
    else:
        shifted(0, 0)
    o_ref[...] = res[:, SHIFT : SHIFT + cols, :].astype(bf16)
    for c in list(direct.values()) + list(relays.values()):
        c.wait_send()


def chunk_of(windows, most):
    return max(d for d in range(1, most + 1) if windows % d == 0) * WIN


def on_device(*args):
    x, labels, rel_index = args[:3]
    qkv_weight, qkv_bias, bias_table, proj_weight = args[5:9]
    fc1_weight, fc1_bias, fc2_weight = args[10:13]
    rows, cols, width = x.shape
    n = lax.axis_size("ch")
    heads = bias_table.shape[2] * n
    args = list(args)
    args[5] = qkv_weight.swapaxes(2, 3)
    args[6] = qkv_bias.swapaxes(0, 1)
    args[7] = bias_table.swapaxes(1, 2)
    hidden = fc1_weight.shape[2] * n
    chunk0, chunk1 = chunk_of(cols // WIN, 4), chunk_of(cols // WIN + 1, 11)
    tall, wide = rows + 2 * SHIFT, cols + 2 * SHIFT
    edge, keys = 16, WIN * WIN
    dma = pltpu.SemaphoreType.DMA
    vm = pltpu.VMEM
    entries = bias_table.shape[1] + -bias_table.shape[1] % 128
    scratch = [
        vm((tall, wide, width), f32), vm((tall, wide, 128), f32), vm((rows, wide, width), f32),
        vm((rows, cols, width), bf16), vm((SHIFT, cols, width), bf16), vm((SHIFT, cols, width), bf16),
        vm((2, rows, edge, width), bf16), vm((2, 2, SHIFT, edge, width), bf16), vm((8, rows, cols), jnp.int32),
        vm((BLOCKS, 8, entries), f32), vm((n, BLOCKS, 8, entries), f32),
        vm((n,) + args[6].shape, f32), vm((n,) + fc1_bias.shape, f32),
        vm((BLOCKS, 3, width, width), bf16), vm((BLOCKS, 1, 3 * width), f32),
        vm((BLOCKS, keys, heads * keys), f32), vm((BLOCKS, width, width), bf16),
        vm((BLOCKS, width, hidden), bf16), vm((BLOCKS, 1, hidden), f32), vm((BLOCKS, hidden, width), bf16),
        dma((n - 1, BLOCKS + 1, 4)), dma((n - 1, BLOCKS + 1, 4)),
        dma((n - 1, BLOCKS, 4)), dma((n - 1, BLOCKS, 4)),
        dma((8,)), dma((8,)), dma((2, cols // chunk0)), dma((2, cols // chunk0)), dma((2, 3)), dma((2, 3)),
        dma((7,)),
    ]
    vmem = pl.BlockSpec(memory_space=vm)
    return pl.pallas_call(
        functools.partial(fused, heads, chunk0, chunk1),
        out_shape=jax.ShapeDtypeStruct(x.shape, bf16),
        in_specs=[vmem] * len(args),
        out_specs=vmem,
        scratch_shapes=scratch,
        compiler_params=pltpu.CompilerParams(
            collective_id=0, has_side_effects=True, vmem_limit_bytes=60 * 1024 * 1024
        ),
        name="fused",
    )(*args)


def solution(mesh):
    in_specs = (
        P(("row", "ch"), "col", None), P(("row", "ch"), "col"), P(), P(), P(),
        P(None, None, None, "ch"), P(None, None, "ch"), P(None, None, "ch"), P(None, "ch", None), P(),
        P(None, None, "ch"), P(None, "ch"), P(None, "ch", None), P(),
    )
    out_specs = P(("row", "ch"), "col", None)
    return jax.shard_map(on_device, mesh=mesh, in_specs=in_specs, out_specs=out_specs, check_vma=False)
```
